128 devices in a mesh: tok: 16 (over x, y_lo, core), own: 8 (over z, y_hi).
Axes of the slice: x: 4, y: 4 (y_hi: 2, y_lo: 2; y = y_hi * 2 + y_lo), z: 4, core: 2. Of those that a mesh axis runs over, the one named last changes fastest.
Arguments:
- expert_ids: int32 [5, 8, 1048576], P(None, None, ('tok', 'own')), may hold values from 0 to 383, as said below
- shard_length: int32 [128], P(('tok', 'own')), may hold values from 2048 to 8192
Outputs:
- lift: float32 [4, 384, 384], P(None, 'own')
The draws below stay inside these ranges and needn't reach their ends.
Inputs may be any that keep to these rules, and one draw needn't show every extreme that they name: For each layer and token slot, expert_ids names 8 different experts.
All inputs are finite; a program needn't handle non-finite values.
Results may differ from the reference program's by a relative error of at most 0.0003.
Values sent between devices are 32-bit elements; how exact they have to be, the bound alone decides.
No kernel may reach another device: no remote copies, remote signals or barrier semaphores. Data moves between devices by JAX's collectives and lax.ppermute only.
A program may use at most 64 MiB of HBM per device.

```python
import math
import jax
import jax.numpy as jnp
from jax import lax

E = 384
K = 8
LAYERS = 5
TOK_DEV = 8192
PAIRS = 4
TOKENS = 1048576
DEVICES = 128


def draw_expert_ids(key, part):
    rows = math.gcd(TOKENS, 8192)
    blocks = TOKENS // rows
    experts = jnp.arange(E, dtype=jnp.int32)

    def one_layer(layer):
        layer_key = jax.random.fold_in(key, 7001 + layer)
        favour = jax.random.randint(jax.random.fold_in(layer_key, 1), (E,), 0, 2 ** 19, dtype=jnp.int32)
        order = jax.random.permutation(jax.random.fold_in(layer_key, 2), experts)
        banned = jnp.any(experts[:, None] == order[None, :3], axis=1)

        def one_block(index):
            block_key = jax.random.fold_in(layer_key, 100 + index)
            noise = jax.random.randint(block_key, (rows, E), 0, 2 ** 20, dtype=jnp.int32)
            score = (noise + favour[None, :]) * E + experts[None, :]
            score = jnp.where(banned[None, :], -1 - experts[None, :], score)
            return lax.top_k(score, K)[1].astype(jnp.int32)
        picked = lax.map(one_block, jnp.arange(blocks, dtype=jnp.int32))
        return jnp.transpose(picked.reshape(TOKENS, K), (1, 0))
    return lax.map(one_layer, jnp.arange(LAYERS, dtype=jnp.int32))


def set_ends(drawn, own_key, smallest, top_value):
    index_at = [jax.random.randint(jax.random.fold_in(own_key, axis), (), 0, length) for axis, length in enumerate(drawn.shape)]
    main_axis = drawn.shape.index(max(drawn.shape))
    neighbour = index_at[:main_axis] + [(index_at[main_axis] + 1) % drawn.shape[main_axis]] + index_at[main_axis + 1:]
    return drawn.at[tuple(index_at)].set(smallest).at[tuple(neighbour)].set(top_value)


def setup_inputs(seed: int = 0) -> dict:
    seeds = jax.random.split(jax.random.key(seed), 3)
    expert_ids = draw_expert_ids(jax.random.fold_in(seeds[2], 71), 0)
    shard_length = set_ends(jax.random.randint(seeds[1], (DEVICES,), TOK_DEV // 4, TOK_DEV + 1), jax.random.fold_in(seeds[1], 1), TOK_DEV // 4, TOK_DEV).astype(jnp.int32)
    return {"expert_ids": expert_ids, "shard_length": shard_length}


def reference(expert_ids, shard_length):
    routes = jnp.transpose(expert_ids, (0, 2, 1))
    position = jnp.arange(TOKENS, dtype=jnp.int32)
    owner = position // TOK_DEV
    live = (position - owner * TOK_DEV < shard_length[owner]).astype(jnp.float32)
    total = jnp.sum(shard_length.astype(jnp.float32))
    weights = jnp.broadcast_to(live[:, None], (TOKENS, K))
    counts = jnp.stack([jnp.zeros((E,), jnp.float32).at[routes[l]].add(weights) for l in range(LAYERS)])
    pair_weights = jnp.broadcast_to(live[:, None, None], (TOKENS, K, K))
    tiles = []
    for p in range(PAIRS):
        index = routes[p][:, :, None] * E + routes[p + 1][:, None, :]
        flat = jnp.zeros((E * E,), jnp.float32).at[index].add(pair_weights)
        tiles.append(flat.reshape(E, E))
    pair_counts = jnp.stack(tiles)
    product = counts[:-1, :, None] * counts[1:, None, :]
    return pair_counts * total / jnp.maximum(product, 1.0)
```

```python
import functools

import jax
import jax.numpy as jnp
import numpy as np
from jax import lax
from jax.experimental import pallas as pl
from jax.experimental.pallas import tpu as pltpu
from jax.sharding import Mesh
from jax.sharding import PartitionSpec as P

E = 384
HOT = jnp.float8_e4m3fn
DEAD = 511
BLOCK = 2048
PIECE = 512
TILES = 40
COUNT_TILE = 36

ALL = ("tok", "own")
AXES = {"x": 4, "yl": 2, "c": 2, "z": 4, "yh": 2}


def groups(axes):
    names = list(AXES)
    rest = [a for a in names if a not in axes]
    order = [names.index(a) for a in rest + list(axes)]
    index = np.arange(128).reshape(tuple(AXES.values()))
    size = int(np.prod([AXES[a] for a in axes]))
    return index.transpose(order).reshape(-1, size).tolist()


def fill_hot(ids, hot, row0):
    tokens = ids.shape[1]
    low = ids & 15
    bit = jnp.left_shift(1, lax.shift_right_logical(ids, 4))
    word = lax.broadcasted_iota(jnp.int32, (16, tokens), 0)
    mask = jnp.zeros((16, tokens), jnp.int32)
    for k in range(ids.shape[0]):
        mask = mask | jnp.where(word == low[k : k + 1], bit[k : k + 1], 0)
    for half in range(2):
        part = (lax.shift_right_logical(mask, 12 * half) & 0xFFF).astype(jnp.int16)
        for b in range(12):
            one = jnp.where((part & jnp.int16(1 << b)) != 0, jnp.bfloat16(1), jnp.bfloat16(0))
            row = row0 + half * 192 + b * 16
            hot[row : row + 16, :] = one.astype(HOT)


def count_pairs(limit, layers, acc, hots, slots):
    steps = slots // BLOCK

    def fill(i, hot):
        for layer, read in enumerate(layers):
            for s in range(0, BLOCK, PIECE):
                start = pl.multiple_of(i * BLOCK + s, PIECE)
                ids = read(start)
                if limit is not None:
                    pos = start + lax.broadcasted_iota(jnp.int32, ids.shape, 1)
                    ids = jnp.where(pos < limit, ids, DEAD)
                fill_hot(ids, hot.at[:, s : s + PIECE], layer * E)

    def multiply(hot):
        acc[...] += lax.dot_general(
            hot[2 * E :, :], hot[: 2 * E, :], (((1,), (1,)), ((), ())), preferred_element_type=jnp.float32
        )

    fill(0, hots[0])

    @pl.loop(0, steps // 2)
    def _(i):
        fill(2 * i + 1, hots[1])
        multiply(hots[0])

        @pl.when(2 * i + 2 < steps)
        def _():
            fill(2 * i + 2, hots[0])

        multiply(hots[1])


def own_kernel(core_ref, limit_ref, a_ref, b_ref, c_ref, acc, hot0, hot1):
    acc[...] = jnp.zeros_like(acc)
    layers = [lambda s, r=r: r[0, :, pl.ds(s, PIECE)] for r in (a_ref, c_ref, b_ref)]
    count_pairs(limit_ref[0], layers, acc, (hot0, hot1), a_ref.shape[2])


def peer_kernel(ids_ref, start_ref, out_ref, acc, hot0, hot1):
    acc[...] = start_ref[...]
    layers = [lambda s, l=l: ids_ref[l, :, pl.ds(s, PIECE)] for l in (0, 2, 1)]
    count_pairs(None, layers, acc, (hot0, hot1), ids_ref.shape[2])
    first = jnp.transpose(acc[:, :E])
    acc[:, :E] = first
    for owner in range(8):
        for pair in range(2):
            for r in range(6):
                for c in range(3):
                    row = 48 * owner + 8 * r
                    col = E * pair + 128 * c
                    out_ref[owner, (pair * 6 + r) * 3 + c] = acc[row : row + 8, col : col + 128]
    count = jnp.sum(acc[...], axis=0, keepdims=True) * 0.125
    rows = [count[:, 128 * i : 128 * i + 128] for i in range(6)] + [jnp.zeros((2, 128), jnp.float32)]
    tile = jnp.concatenate(rows, axis=0)
    for owner in range(8):
        out_ref[owner, COUNT_TILE] = tile
        out_ref[owner, COUNT_TILE + 1 :] = jnp.zeros((TILES - COUNT_TILE - 1, 8, 128), jnp.float32)


def lift_kernel(core_ref, mine_ref, other_ref, out_ref):
    core = core_ref[0]
    for half, ref in ((core, mine_ref), (1 - core, other_ref)):
        counts = ref[COUNT_TILE]
        total = jnp.sum(counts[0:3, :]) * 0.125
        for pair in range(2):
            for r in range(6):
                base = (pair * 6 + r) * 3
                tiles = [ref[base + c] for c in range(3)]
                left = jnp.sum(tiles[0] + tiles[1] + tiles[2], axis=1, keepdims=True) * 0.125
                for c in range(3):
                    right = counts[3 * pair + c : 3 * pair + c + 1, :]
                    value = tiles[c] * total / jnp.maximum(left * right, 1.0)
                    out_ref[2 * half + pair, 8 * r : 8 * r + 8, 128 * c : 128 * c + 128] = value


def shards(expert_ids, shard_length):
    slots = expert_ids.shape[2]
    core = lax.axis_index("tok") & 1
    core_arg = core.reshape(1).astype(jnp.int32)
    live = lax.broadcasted_iota(jnp.int32, (1, 1, slots), 2) < shard_length[0]
    send = lax.dynamic_slice_in_dim(expert_ids, 2 * (1 - core), 3, 0)
    send = jnp.where(live, send, DEAD)
    peer = lax.ppermute(send, ALL, [(i, i ^ 8) for i in range(128)])

    params = pltpu.CompilerParams(vmem_limit_bytes=32 * 1024 * 1024)
    flops = 2 * slots * E * 2 * E
    hots = [pltpu.VMEM((3 * E, BLOCK), HOT)] * 2
    layer = lambda k: pl.BlockSpec((1, 8, slots), lambda i, c: (2 * c[0] + k, 0, 0))
    start = pl.pallas_call(
        own_kernel,
        grid_spec=pltpu.PrefetchScalarGridSpec(
            num_scalar_prefetch=1,
            grid=(1,),
            in_specs=[pl.BlockSpec(memory_space=pltpu.SMEM), layer(0), layer(1), layer(2)],
            out_specs=pl.BlockSpec((E, 2 * E), lambda i, c: (0, 0)),
            scratch_shapes=hots,
        ),
        out_shape=jax.ShapeDtypeStruct((E, 2 * E), jnp.float32),
        compiler_params=params,
        cost_estimate=pl.CostEstimate(flops=flops, bytes_accessed=2 << 20, transcendentals=0),
        name="own_tokens",
    )(core_arg, shard_length, expert_ids, expert_ids, expert_ids)
    chunk = pl.pallas_call(
        peer_kernel,
        out_shape=jax.ShapeDtypeStruct((8, TILES, 8, 128), jnp.float32),
        scratch_shapes=[pltpu.VMEM((E, 2 * E), jnp.float32)] + hots,
        compiler_params=params,
        cost_estimate=pl.CostEstimate(flops=flops, bytes_accessed=2 << 20, transcendentals=0),
        name="peer_tokens",
    )(peer, start)

    parts = chunk.reshape(64, TILES, 128)
    parts = lax.all_to_all(
        parts, ALL, 0, 0, axis_index_groups=groups(["z", "yh", "x", "yl"]), tiled=True
    )
    piece = parts.sum(axis=0)
    spread = jnp.broadcast_to(piece[None], (8, TILES, 128))
    whole = lax.all_to_all(spread, ALL, 0, 0, axis_index_groups=groups(["x", "yl"]), tiled=True)
    mine = whole.reshape(TILES, 8, 128)
    other = lax.ppermute(mine, ALL, [(i, i ^ 8) for i in range(128)])
    return pl.pallas_call(
        lift_kernel,
        in_specs=[pl.BlockSpec(memory_space=pltpu.SMEM)] + [pl.BlockSpec(memory_space=pltpu.VMEM)] * 2,
        out_shape=jax.ShapeDtypeStruct((4, E // 8, E), jnp.float32),
        name="lift",
    )(core_arg, mine, other)


def solution(mesh):
    torus = Mesh(mesh.devices.reshape(16, 8), ALL)
    return jax.shard_map(
        shards,
        mesh=torus,
        in_specs=(P(None, None, ALL), P(ALL)),
        out_specs=P(None, "own", None),
        check_vma=False,
    )
```

```python
import functools

import jax
import jax.numpy as jnp
import numpy as np
from jax import lax
from jax.experimental import pallas as pl
from jax.experimental.pallas import tpu as pltpu
from jax.sharding import Mesh
from jax.sharding import PartitionSpec as P

E = 384
HOT = jnp.float8_e4m3fn
DEAD = 511
BLOCK = 2048
PIECE = 512
TILES = 40
COUNT_TILE = 36

ALL = ("tok", "own")
AXES = {"x": 4, "yl": 2, "c": 2, "z": 4, "yh": 2}


def groups(axes):
    names = list(AXES)
    rest = [a for a in names if a not in axes]
    order = [names.index(a) for a in rest + list(axes)]
    index = np.arange(128).reshape(tuple(AXES.values()))
    size = int(np.prod([AXES[a] for a in axes]))
    return index.transpose(order).reshape(-1, size).tolist()


def fill_hot(ids, hot, row0):
    tokens = ids.shape[1]
    low = ids & 15
    bit = jnp.left_shift(1, lax.shift_right_logical(ids, 4))
    word = lax.broadcasted_iota(jnp.int32, (16, tokens), 0)
    mask = jnp.zeros((16, tokens), jnp.int32)
    one, zero = jnp.bfloat16(1), jnp.bfloat16(0)
    for k in range(ids.shape[0]):
        mask = mask | jnp.where(word == low[k : k + 1], bit[k : k + 1], 0)
    for half in range(2):
        part = (lax.shift_right_logical(mask, 12 * half) & 0xFFF).astype(jnp.int16)
        for b in range(0, 12, 2):
            ones = [jnp.where((part & jnp.int16(1 << n)) != 0, one, zero) for n in (b, b + 1)]
            row = row0 + half * 192 + b * 16
            hot[row : row + 32, :] = jnp.concatenate(ones, axis=0).astype(HOT)


def add_pairs(core, limit, ids_ref, acc, hot):
    @pl.loop(0, ids_ref.shape[2] // BLOCK)
    def _(i):
        for place, layer in enumerate((0, 2, 1)):
            for s in range(0, BLOCK, PIECE):
                start = pl.multiple_of(i * BLOCK + s, PIECE)
                ids = ids_ref[2 * core + layer, :, pl.ds(start, PIECE)]
                slot = start + lax.broadcasted_iota(jnp.int32, ids.shape, 1)
                ids = jnp.where(slot < limit, ids, DEAD)
                fill_hot(ids, hot.at[:, s : s + PIECE], place * E)
        acc[...] += lax.dot_general(
            hot[2 * E :, :], hot[: 2 * E, :], (((1,), (1,)), ((), ())), preferred_element_type=jnp.float32
        )


def own_kernel(core_ref, limit_ref, ids_ref, acc, hot):
    acc[...] = jnp.zeros_like(acc)
    add_pairs(core_ref[0], limit_ref[0], ids_ref, acc, hot)


def peer_kernel(core_ref, limit_ref, ids_ref, start_ref, out_ref, acc, hot):
    acc[...] = start_ref[...]
    add_pairs(core_ref[0], limit_ref[0], ids_ref, acc, hot)
    count = jnp.sum(acc[...], axis=0, keepdims=True) * 0.125
    acc[:, :E] = jnp.transpose(acc[:, :E])
    for owner in range(8):
        for pair in range(2):
            for r in range(6):
                for c in range(3):
                    row = 48 * owner + 8 * r
                    col = E * pair + 128 * c
                    out_ref[owner, (pair * 6 + r) * 3 + c] = acc[row : row + 8, col : col + 128]
    count_b = jnp.sum(acc[:, :E], axis=0, keepdims=True) * 0.125
    rows = [count_b[:, 128 * i : 128 * i + 128] for i in range(3)]
    rows += [count[:, E + 128 * i : E + 128 * i + 128] for i in range(3)]
    tile = jnp.concatenate(rows + [jnp.zeros((2, 128), jnp.float32)], axis=0)
    for owner in range(8):
        out_ref[owner, COUNT_TILE] = tile
        out_ref[owner, COUNT_TILE + 1 :] = jnp.zeros((TILES - COUNT_TILE - 1, 8, 128), jnp.float32)


def lift_kernel(core_ref, mine_ref, other_ref, out_ref):
    core = core_ref[0]
    for half, ref in ((core, mine_ref), (1 - core, other_ref)):
        counts = ref[COUNT_TILE]
        total = jnp.sum(counts[0:3, :]) * 0.125
        for pair in range(2):
            for r in range(6):
                base = (pair * 6 + r) * 3
                tiles = [ref[base + c] for c in range(3)]
                left = jnp.sum(tiles[0] + tiles[1] + tiles[2], axis=1, keepdims=True) * 0.125
                for c in range(3):
                    right = counts[3 * pair + c : 3 * pair + c + 1, :]
                    value = tiles[c] * total / jnp.maximum(left * right, 1.0)
                    out_ref[2 * half + pair, 8 * r : 8 * r + 8, 128 * c : 128 * c + 128] = value


def shards(expert_ids, shard_length):
    slots = expert_ids.shape[2]
    core = (lax.axis_index("tok") & 1).reshape(1).astype(jnp.int32)
    swap = [(i, i ^ 8) for i in range(128)]
    peer_ids = lax.ppermute(expert_ids, ALL, swap)
    peer_limit = lax.ppermute(shard_length, ALL, swap)

    params = pltpu.CompilerParams(vmem_limit_bytes=24 * 1024 * 1024)
    flops = 2 * slots * E * 2 * E
    smem = pl.BlockSpec(memory_space=pltpu.SMEM)
    vmem = pl.BlockSpec(memory_space=pltpu.VMEM)
    hot = pltpu.VMEM((3 * E, BLOCK), HOT)
    start = pl.pallas_call(
        own_kernel,
        in_specs=[smem, smem, vmem],
        out_specs=vmem,
        out_shape=jax.ShapeDtypeStruct((E, 2 * E), jnp.float32),
        scratch_shapes=[hot],
        compiler_params=params,
        cost_estimate=pl.CostEstimate(flops=flops, bytes_accessed=2 << 20, transcendentals=0),
        name="own_tokens",
    )(core, shard_length, expert_ids)
    chunk = pl.pallas_call(
        peer_kernel,
        in_specs=[smem, smem, vmem, vmem],
        out_specs=vmem,
        out_shape=jax.ShapeDtypeStruct((8, TILES, 8, 128), jnp.float32),
        scratch_shapes=[pltpu.VMEM((E, 2 * E), jnp.float32), hot],
        compiler_params=params,
        cost_estimate=pl.CostEstimate(flops=flops, bytes_accessed=2 << 20, transcendentals=0),
        name="peer_tokens",
    )(core, peer_limit, peer_ids, start)

    half = TILES // 2
    parts = lax.all_to_all(
        chunk.reshape(16, 8 * half, 128), ALL, 0, 0, axis_index_groups=groups(["z", "yh", "yl"]), tiled=True
    )
    piece = parts.sum(axis=0)
    spread = jnp.broadcast_to(piece[None], (8, 8 * half, 128))
    whole = lax.all_to_all(spread, ALL, 0, 0, axis_index_groups=groups(["x", "yl"]), tiled=True)
    mine = whole.reshape(4, TILES, 8, 128).sum(axis=0)
    other = lax.ppermute(mine, ALL, swap)
    return pl.pallas_call(
        lift_kernel,
        in_specs=[smem, vmem, vmem],
        out_specs=vmem,
        out_shape=jax.ShapeDtypeStruct((4, E // 8, E), jnp.float32),
        compiler_params=pltpu.CompilerParams(vmem_limit_bytes=8 * 1024 * 1024),
        name="lift",
    )(core, mine, other)


def solution(mesh):
    torus = Mesh(mesh.devices.reshape(16, 8), ALL)
    return jax.shard_map(
        shards,
        mesh=torus,
        in_specs=(P(None, None, ALL), P(ALL)),
        out_specs=P(None, "own", None),
        check_vma=False,
    )
```
